128 devices in a mesh: dp: 1, sp: 16 (over z, y), tp: 8 (over x, core).
Axes of the slice: x: 4, y: 4, z: 4, core: 2. Of those that a mesh axis runs over, the one named last changes fastest.
Arguments:
- hidden_in: bfloat16 [4096, 5120], P(('dp', 'sp', 'tp'))
- segment_ids: int32 [4096], P(('dp', 'sp', 'tp'))
- positions: int32 [4096], P(('dp', 'sp', 'tp'))
- attn_gain: bfloat16 [2, 5120], replicated
- w_q: bfloat16 [2, 5120, 4096], P(None, None, 'tp')
- w_k: bfloat16 [2, 5120, 1024], P(None, None, 'tp')
- w_v: bfloat16 [2, 5120, 1024], P(None, None, 'tp')
- w_o: bfloat16 [2, 4096, 5120], P(None, 'tp')
- mlp_gain: bfloat16 [2, 5120], replicated
- w_gate: bfloat16 [2, 5120, 14336], P(None, None, 'tp')
- w_up: bfloat16 [2, 5120, 14336], P(None, None, 'tp')
- w_down: bfloat16 [2, 14336, 5120], P(None, 'tp')
Outputs:
- output 1: bfloat16 [4096, 5120], P(('dp', 'sp', 'tp'))
- output 2: bfloat16 [2, 4096, 8, 128], P(None, ('dp', 'sp'), 'tp')
- output 3: bfloat16 [2, 4096, 8, 128], P(None, ('dp', 'sp'), 'tp')
All inputs are finite; a program needn't handle non-finite values.
Results may differ from the reference program's by a relative error of at most 0.0178663.
Values are sent between devices in bfloat16 or wider.
A program may use at most 1 GiB of HBM per device.

```python
import math
import jax
import jax.numpy as jnp
from jax import lax

TOKENS = 4096
MODEL_DIM = 5120
HEADS = 32
KV_HEADS = 8
HEAD_DIM = 128
FFN_DIM = 14336
LAYERS = 2
SEGMENTS = 4

GROUP = HEADS // KV_HEADS
Q_BLOCK = math.gcd(TOKENS, 32)
ROPE_BASE = 1e4
NORM_EPS = 1e-5
SCORE_SCALE = HEAD_DIM ** -0.5


def setup_inputs(seed: int = 0, part: int = 0) -> dict:
    part_key = jax.random.fold_in(jax.random.key(seed), part)
    act_keys = jax.random.split(part_key, 6)
    base_noise = jax.random.normal(act_keys[0], (TOKENS, MODEL_DIM), jnp.float32)
    cycles = jax.random.uniform(act_keys[1], (MODEL_DIM,), jnp.float32, 0.5, 3.0)
    phases = jax.random.uniform(act_keys[2], (MODEL_DIM,), jnp.float32, 0.0, 6.2832)
    time_ramp = jnp.arange(TOKENS, dtype=jnp.float32) / TOKENS
    drift_part = jnp.cos(6.2832 * time_ramp[:, None] * cycles[None, :] + phases[None, :])
    hidden_in = (0.6 * base_noise + 1.2 * drift_part).astype(jnp.bfloat16)
    cut_points = jax.random.permutation(act_keys[3], TOKENS - 1)[: SEGMENTS - 1] + 1
    seg_marks = jnp.zeros((TOKENS,), jnp.int32).at[cut_points].set(1)
    segment_ids = jnp.cumsum(seg_marks).astype(jnp.int32)
    pos_steps = jax.random.randint(act_keys[4], (TOKENS,), 1, 3)
    pos_start = jax.random.randint(act_keys[5], (), 0, 64)
    positions = (jnp.cumsum(pos_steps) + pos_start).astype(jnp.int32)
    w_keys = jax.random.split(jax.random.key(seed + 1), 9)

    def normal_w(key_w, shape_w, scale_w):
        return (jax.random.normal(key_w, shape_w, jnp.float32) * scale_w).astype(jnp.bfloat16)

    def gain_w(key_w):
        return (1.0 + 0.3 * jax.random.normal(key_w, (LAYERS, MODEL_DIM), jnp.float32)).astype(jnp.bfloat16)

    dim_scale = MODEL_DIM ** -0.5
    return {
        'hidden_in': hidden_in,
        'segment_ids': segment_ids,
        'positions': positions,
        'attn_gain': gain_w(w_keys[0]),
        'w_q': normal_w(w_keys[1], (LAYERS, MODEL_DIM, HEADS * HEAD_DIM), 1.4 * dim_scale),
        'w_k': normal_w(w_keys[2], (LAYERS, MODEL_DIM, KV_HEADS * HEAD_DIM), 1.4 * dim_scale),
        'w_v': normal_w(w_keys[3], (LAYERS, MODEL_DIM, KV_HEADS * HEAD_DIM), dim_scale),
        'w_o': normal_w(w_keys[4], (LAYERS, HEADS * HEAD_DIM, MODEL_DIM), 0.7 * (HEADS * HEAD_DIM) ** -0.5),
        'mlp_gain': gain_w(w_keys[5]),
        'w_gate': normal_w(w_keys[6], (LAYERS, MODEL_DIM, FFN_DIM), dim_scale),
        'w_up': normal_w(w_keys[7], (LAYERS, MODEL_DIM, FFN_DIM), dim_scale),
        'w_down': normal_w(w_keys[8], (LAYERS, FFN_DIM, MODEL_DIM), 0.7 * FFN_DIM ** -0.5),
    }


def rms_norm(hidden, gain_vec):
    hidden32 = hidden.astype(jnp.float32)
    inv_rms = lax.rsqrt(jnp.mean(hidden32 * hidden32, axis=-1, keepdims=True) + NORM_EPS)
    return (hidden32 * inv_rms * gain_vec.astype(jnp.float32)).astype(jnp.bfloat16)


def rotary(rot_in, positions):
    half_dim = HEAD_DIM // 2
    inv_freq = ROPE_BASE ** (-jnp.arange(half_dim, dtype=jnp.float32) / half_dim)
    angles = positions.astype(jnp.float32)[..., None] * inv_freq
    cos_val = jnp.cos(angles)[..., None, :]
    sin_val = jnp.sin(angles)[..., None, :]
    first_half = rot_in[..., :half_dim]
    second_half = rot_in[..., half_dim:]
    return jnp.concatenate([first_half * cos_val - second_half * sin_val, second_half * cos_val + first_half * sin_val], axis=-1)


def attention(q_rot, k_rot, v_val, segment_ids):
    n_blocks = TOKENS // Q_BLOCK
    key_index = jnp.arange(TOKENS)
    k_wide = k_rot.astype(jnp.float32)
    v_wide = v_val.astype(jnp.float32)

    def one_block(block_in):
        q_blk, idx_blk, seg_blk = block_in
        scores = jnp.einsum('qkgd,skd->kgqs', q_blk.astype(jnp.float32), k_wide) * SCORE_SCALE
        allowed = (idx_blk[:, None] >= key_index[None, :]) & (seg_blk[:, None] == segment_ids[None, :])
        probs = jax.nn.softmax(jnp.where(allowed, scores, -1e30), axis=-1).astype(jnp.bfloat16)
        return jnp.einsum('kgqs,skd->qkgd', probs.astype(jnp.float32), v_wide).astype(jnp.bfloat16)

    blocks = (q_rot.reshape(n_blocks, Q_BLOCK, KV_HEADS, GROUP, HEAD_DIM),
              key_index.reshape(n_blocks, Q_BLOCK), segment_ids.reshape(n_blocks, Q_BLOCK))
    return lax.map(one_block, blocks).reshape(TOKENS, HEADS * HEAD_DIM)


def reference(hidden_in, segment_ids, positions, attn_gain, w_q, w_k, w_v, w_o, mlp_gain, w_gate, w_up, w_down):
    def layer_step(hidden, layer_w):
        gain_attn, wq_l, wk_l, wv_l, wo_l, gain_mlp, wg_l, wu_l, wd_l = layer_w
        normed = rms_norm(hidden, gain_attn)
        q_lin = jnp.dot(normed, wq_l, preferred_element_type=jnp.float32).reshape(TOKENS, HEADS, HEAD_DIM)
        k_lin = jnp.dot(normed, wk_l, preferred_element_type=jnp.float32).reshape(TOKENS, KV_HEADS, HEAD_DIM)
        v_val = jnp.dot(normed, wv_l, preferred_element_type=jnp.float32).astype(jnp.bfloat16).reshape(TOKENS, KV_HEADS, HEAD_DIM)
        q_rot = rotary(q_lin, positions).astype(jnp.bfloat16).reshape(TOKENS, KV_HEADS, GROUP, HEAD_DIM)
        k_rot = rotary(k_lin, positions).astype(jnp.bfloat16)
        att_out = attention(q_rot, k_rot, v_val, segment_ids)
        proj_out = jnp.dot(att_out, wo_l, preferred_element_type=jnp.float32).astype(jnp.bfloat16)
        hidden_mid = (hidden.astype(jnp.float32) + proj_out.astype(jnp.float32)).astype(jnp.bfloat16)
        normed_mlp = rms_norm(hidden_mid, gain_mlp)
        gate_lin = jnp.dot(normed_mlp, wg_l, preferred_element_type=jnp.float32)
        up_lin = jnp.dot(normed_mlp, wu_l, preferred_element_type=jnp.float32)
        act_vals = (jax.nn.silu(gate_lin) * up_lin).astype(jnp.bfloat16)
        down_out = jnp.dot(act_vals, wd_l, preferred_element_type=jnp.float32).astype(jnp.bfloat16)
        hidden_new = (hidden_mid.astype(jnp.float32) + down_out.astype(jnp.float32)).astype(jnp.bfloat16)
        return hidden_new, (k_rot, v_val)

    hidden_out, caches = lax.scan(layer_step, hidden_in, (attn_gain, w_q, w_k, w_v, w_o, mlp_gain, w_gate, w_up, w_down))
    return hidden_out, caches[0], caches[1]
```

```python
import functools
import math
import jax
import jax.numpy as jnp
from jax import lax
from jax.experimental import pallas as pl
from jax.experimental.pallas import tpu as pltpu
from jax.sharding import PartitionSpec as P

HEAD_DIM = 128
ROPE_BASE = 1e4
NORM_EPS = 1e-5
SCORE_SCALE = HEAD_DIM ** -0.5
NX = 4
AG_AHEAD = 4
AG_LAG_O = 3
AG_LAG = 5
RS_LAG_D = 2
RS_LAG_T = 5
RS_LAG_F = 8
WG_SLOTS = 4
WD_SLOTS = 4
MESH = pl.DeviceIdType.MESH
F32 = jnp.float32
BF16 = jnp.bfloat16


class Ring:
    def __init__(self):
        tp = lax.axis_index('tp')
        self.tp = tp
        self.x = lax.div(tp, 2)
        self.c = lax.rem(tp, 2)

    def dev(self, dx, same_core=True):
        core = self.c if same_core else 1 - self.c
        return {'tp': 2 * self.at(dx) + core}

    def at(self, dx):
        return lax.rem(self.x + dx + NX, NX)


def col(ref, j, width):
    return ref.at[:, pl.ds(pl.multiple_of(j * width, width), width)]


class Gather:
    def __init__(self, ring, buf, send, recv, rows, nch):
        self.g, self.buf, self.send, self.recv, self.rows, self.nch = ring, buf, send, recv, rows, nch

    def block(self, j, dx, same_core):
        core = self.g.c if same_core else 1 - self.g.c
        r = pl.multiple_of((2 * self.g.at(dx) + core) * self.rows, self.rows)
        return self.buf.at[j, pl.ds(r, self.rows), :]

    def copy(self, j, kind, dx, to):
        ref = self.block(j, dx, True)
        return pltpu.make_async_remote_copy(src_ref=ref, dst_ref=ref, send_sem=self.send.at[kind, j], recv_sem=self.recv.at[kind, j],
                                            device_id=to, device_id_type=MESH)

    def arrival(self, j, kind, dx, same_core):
        ref = self.block(j, dx, same_core)
        return pltpu.make_async_remote_copy(src_ref=ref, dst_ref=ref, send_sem=self.send.at[kind, j], recv_sem=self.recv.at[kind, j],
                                            device_id=self.g.dev(0, False), device_id_type=MESH)

    def start(self, j):
        self.copy(j, 0, 0, self.g.dev(1)).start()
        self.copy(j, 1, 0, self.g.dev(-1)).start()
        self.copy(j, 3, 0, self.g.dev(0, False)).start()

    def forward(self, j):
        self.arrival(j, 0, -1, True).wait_recv()
        self.arrival(j, 1, 1, True).wait_recv()
        way = 1 - 2 * lax.rem(j, 2)
        self.copy(j, 2, -way, self.g.dev(way)).start()
        self.copy(j, 4, -1, self.g.dev(0, False)).start()
        self.copy(j, 5, 1, self.g.dev(0, False)).start()

    def forward_far(self, j):
        self.arrival(j, 2, 2, True).wait_recv()
        self.copy(j, 6, 2, self.g.dev(0, False)).start()

    def whole(self, j):
        self.arrival(j, 3, 0, False).wait_recv()
        self.arrival(j, 4, -1, False).wait_recv()
        self.arrival(j, 5, 1, False).wait_recv()
        self.arrival(j, 6, 2, False).wait_recv()

    def drain(self):
        def body(j, _):
            for kind in range(7):
                self.arrival(j, kind, 0, True).wait_send()
            return 0
        lax.fori_loop(0, self.nch, body, 0)

    def run(self, use, last=None):
        nch = self.nch
        for j in range(min(AG_AHEAD, nch)):
            self.start(j)

        def body(s, _):
            @pl.when(s < nch)
            def _():
                self.forward(s)

            @pl.when(s + AG_AHEAD < nch)
            def _():
                self.start(s + AG_AHEAD)

            @pl.when((s >= AG_LAG_O) & (s - AG_LAG_O < nch))
            def _():
                self.forward_far(s - AG_LAG_O)

            @pl.when(s >= AG_LAG)
            def _():
                self.whole(s - AG_LAG)
                use(s - AG_LAG)
            return 0
        stop = nch if last is None else nch - 1
        lax.fori_loop(0, stop + AG_LAG, body, 0)
        if last is not None:
            self.whole(nch - 1)
            last()
        self.drain()


class Scatter:
    def __init__(self, ring, part, pair, passing, ends, own, out, send, recv, nch):
        self.g, self.part, self.pair, self.passing, self.ends, self.own, self.out = ring, part, pair, passing, ends, own, out
        self.send, self.recv, self.nch = send, recv, nch

    def remote(self, j, kind, src, dst, to):
        return pltpu.make_async_remote_copy(src_ref=src, dst_ref=dst, send_sem=self.send.at[kind, j], recv_sem=self.recv.at[kind, j],
                                            device_id=to, device_id_type=MESH)

    def pair_copy(self, j):
        return self.remote(j, 0, self.part.at[j, :, 1 - self.g.c], self.pair.at[j], self.g.dev(0, False))

    def far_copy(self, j):
        way = 1 - 2 * lax.rem(j, 2)
        return self.remote(j, 1, self.out.at[j, 2], self.passing.at[j], self.g.dev(way))

    def near_copy(self, j, side):
        return self.remote(j, 2 + side, self.out.at[j, side], self.ends.at[j, side], self.g.dev(1 - 2 * side))

    def near_now(self, j, odd):
        self.near_copy(j, 1 - odd).start()

    def stage_pair(self, j):
        self.pair_copy(j).wait_recv()
        g = self.g

        def both(dx):
            xx = g.at(dx)
            return self.part[j, xx, g.c].astype(F32) + self.pair[j, xx].astype(F32)
        self.out[j, 2] = both(2).astype(BF16)
        self.far_copy(j).start()
        self.out[j, 0] = both(1).astype(BF16)
        self.out[j, 1] = both(-1).astype(BF16)
        side = 1 - lax.rem(j, 2)
        pltpu.make_async_remote_copy(src_ref=self.out.at[j, side], dst_ref=self.ends.at[j, side], send_sem=self.send.at[2, j],
                                     recv_sem=self.recv.at[2, j], device_id=g.dev(1 - 2 * side), device_id_type=MESH).start()
        self.own[j] = both(0)

    def stage_pass(self, j):
        g = self.g
        self.far_copy(j).wait_recv()
        side = lax.rem(j, 2)
        self.out[j, side] = (self.out[j, side].astype(F32) + self.passing[j].astype(F32)).astype(BF16)
        pltpu.make_async_remote_copy(src_ref=self.out.at[j, side], dst_ref=self.ends.at[j, side], send_sem=self.send.at[3, j],
                                     recv_sem=self.recv.at[3, j], device_id=g.dev(1 - 2 * side), device_id_type=MESH).start()

    def stage_end(self, j):
        for kind in (2, 3):
            self.remote(j, kind, self.ends.at[j, 0], self.ends.at[j, 0], self.g.dev(1)).wait_recv()
        return self.own[j] + self.ends[j, 0].astype(F32) + self.ends[j, 1].astype(F32)

    def drain(self):
        def body(j, _):
            self.pair_copy(j).wait_send()
            for kind in (1, 2, 3):
                self.remote(j, kind, self.ends.at[j, 0], self.ends.at[j, 0], self.g.dev(1)).wait_send()
            return 0
        lax.fori_loop(0, self.nch, body, 0)

    def run(self, compute, finish):
        nch = self.nch

        def body(s, _):
            @pl.when(s < nch)
            def _():
                self.part[s] = compute(s)
                self.pair_copy(s).start()

            @pl.when((s >= RS_LAG_D) & (s - RS_LAG_D < nch))
            def _():
                self.stage_pair(s - RS_LAG_D)

            @pl.when((s >= RS_LAG_T) & (s - RS_LAG_T < nch))
            def _():
                self.stage_pass(s - RS_LAG_T)

            @pl.when(s >= RS_LAG_F)
            def _():
                j = s - RS_LAG_F
                finish(j, self.stage_end(j))
            return 0
        lax.fori_loop(0, nch + RS_LAG_F, body, 0)
        self.drain()


def enter(peers):
    barrier = pltpu.get_barrier_semaphore()
    for dev in peers:
        pl.semaphore_signal(barrier, inc=1, device_id=dev, device_id_type=MESH)
    pl.semaphore_wait(barrier, len(peers))


def mlp_kernel(layer, dims, h_hbm, gain_ref, wg_hbm, wu_hbm, wd_hbm, out_ref,
               h_ref, nbuf, acc_g, acc_u, act, wgu, wd, part, pair, passing, ends, own, outs,
               h_sem, w_sem, d_sem, ag_send, ag_recv, rs_send, rs_recv):
    rows, d_model, units, nch = dims
    cw = d_model // nch
    g = Ring()
    h_in = pltpu.make_async_copy(h_hbm, h_ref, h_sem)
    h_in.start()

    def gu_copy(j, k):
        slot = lax.rem(j, WG_SLOTS)
        src = (wg_hbm, wu_hbm)[k]
        return pltpu.make_async_copy(src.at[layer, pl.ds(pl.multiple_of(j * cw, cw), cw), :], wgu.at[slot, k], w_sem.at[slot, k])

    def d_copy(j):
        slot = lax.rem(j, WD_SLOTS)
        return pltpu.make_async_copy(wd_hbm.at[layer, :, pl.ds(pl.multiple_of(j * cw, cw), cw)], wd.at[slot], d_sem.at[slot])
    for j in range(WG_SLOTS):
        gu_copy(j, 0).start()
        gu_copy(j, 1).start()
    for j in range(WD_SLOTS):
        d_copy(j).start()
    enter([g.dev(1), g.dev(-1), g.dev(0, False)])
    h_in.wait()

    h32 = h_ref[...].astype(F32)
    inv = lax.rsqrt(jnp.mean(h32 * h32, axis=-1, keepdims=True) + NORM_EPS)
    me = pl.ds(pl.multiple_of(g.tp * rows, rows), rows)
    for j in range(nch):
        sl = slice(j * cw, (j + 1) * cw)
        nbuf[j, me, :] = (h_ref[:, sl].astype(F32) * inv * gain_ref[layer:layer + 1, sl].astype(F32)).astype(BF16)
    acc_g[...] = jnp.zeros_like(acc_g)
    acc_u[...] = jnp.zeros_like(acc_u)

    def gate_up(j):
        slot = lax.rem(j, WG_SLOTS)
        for k, acc in ((0, acc_g), (1, acc_u)):
            gu_copy(j, k).wait()
            acc[...] += jnp.dot(nbuf[j], wgu[slot, k], preferred_element_type=F32)

            @pl.when(j + WG_SLOTS < nch)
            def _():
                gu_copy(j + WG_SLOTS, k).start()

    def gate_up_last():
        j = nch - 1
        slot = j % WG_SLOTS
        gu_copy(j, 0).wait()
        gu_copy(j, 1).wait()
        step = min(256, units)
        for t in range(0, units, step):
            sl = slice(t, t + step)
            gate = acc_g[:, sl] + jnp.dot(nbuf[j], wgu[slot, 0, :, sl], preferred_element_type=F32)
            up = acc_u[:, sl] + jnp.dot(nbuf[j], wgu[slot, 1, :, sl], preferred_element_type=F32)
            act[:, sl] = (gate * jax.nn.sigmoid(gate) * up).astype(BF16)

    Gather(g, nbuf, ag_send, ag_recv, rows, nch).run(gate_up, gate_up_last)

    def down(j):
        d_copy(j).wait()
        slot = lax.rem(j, WD_SLOTS)
        res = jnp.dot(act[...], wd[slot], preferred_element_type=F32).astype(BF16)

        @pl.when(j + WD_SLOTS < nch)
        def _():
            d_copy(j + WD_SLOTS).start()
        return res.reshape(NX, 2, rows, cw)

    def finish(j, total):
        h_col = col(h_ref, j, cw)
        col(out_ref, j, cw)[...] = (h_col[...].astype(F32) + total.astype(BF16).astype(F32)).astype(BF16)

    Scatter(g, part, pair, passing, ends, own, outs, rs_send, rs_recv, nch).run(down, finish)


def mlp_call(layer, hidden, gain, w_gate, w_up, w_down, nch=10):
    rows, d_model = hidden.shape
    units = w_gate.shape[2]
    cw = d_model // nch
    tokens = rows * NX * 2
    any_spec = pl.BlockSpec(memory_space=pl.ANY)
    vmem = pl.BlockSpec(memory_space=pltpu.VMEM)
    dma = pltpu.SemaphoreType.DMA
    return pl.pallas_call(
        functools.partial(mlp_kernel, layer, (rows, d_model, units, nch)),
        out_shape=jax.ShapeDtypeStruct((rows, d_model), BF16),
        in_specs=[any_spec, vmem, any_spec, any_spec, any_spec],
        out_specs=vmem,
        scratch_shapes=[
            pltpu.VMEM((rows, d_model), BF16),
            pltpu.VMEM((nch, tokens, cw), BF16),
            pltpu.VMEM((tokens, units), F32),
            pltpu.VMEM((tokens, units), F32),
            pltpu.VMEM((tokens, units), BF16),
            pltpu.VMEM((WG_SLOTS, 2, cw, units), BF16),
            pltpu.VMEM((WD_SLOTS, units, cw), BF16),
            pltpu.VMEM((nch, NX, 2, rows, cw), BF16),
            pltpu.VMEM((nch, NX, rows, cw), BF16),
            pltpu.VMEM((nch, rows, cw), BF16),
            pltpu.VMEM((nch, 2, rows, cw), BF16),
            pltpu.VMEM((nch, rows, cw), F32),
            pltpu.VMEM((nch, 3, rows, cw), BF16),
            dma, dma((WG_SLOTS, 2)), dma((WD_SLOTS,)),
            dma((7, nch)), dma((7, nch)), dma((4, nch)), dma((4, nch)),
        ],
        compiler_params=pltpu.CompilerParams(collective_id=0, has_side_effects=True, vmem_limit_bytes=62 * 1024 * 1024),
        name='mlp',
    )(hidden, gain, w_gate, w_up, w_down)


def rms_norm(hidden, gain_vec):
    hidden32 = hidden.astype(jnp.float32)
    inv_rms = lax.rsqrt(jnp.mean(hidden32 * hidden32, axis=-1, keepdims=True) + NORM_EPS)
    return (hidden32 * inv_rms * gain_vec.astype(jnp.float32)).astype(jnp.bfloat16)


def rotary(rot_in, positions):
    half_dim = HEAD_DIM // 2
    inv_freq = ROPE_BASE ** (-jnp.arange(half_dim, dtype=jnp.float32) / half_dim)
    angles = positions.astype(jnp.float32)[..., None] * inv_freq
    cos_val = jnp.cos(angles)[..., None, :]
    sin_val = jnp.sin(angles)[..., None, :]
    first_half = rot_in[..., :half_dim]
    second_half = rot_in[..., half_dim:]
    return jnp.concatenate([first_half * cos_val - second_half * sin_val, second_half * cos_val + first_half * sin_val], axis=-1)


def attention_rows(q_rot, k_keys, v_keys, row_index, row_seg, key_seg):
    n_rows, n_kv, group_size = q_rot.shape[0], q_rot.shape[1], q_rot.shape[2]
    blk_rows = math.gcd(n_rows, 128)
    n_blocks = n_rows // blk_rows
    key_index = jnp.arange(k_keys.shape[0])

    def one_block(block_in):
        q_blk, idx_blk, seg_blk = block_in
        scores = jnp.einsum('qkgd,skd->kgqs', q_blk, k_keys, preferred_element_type=jnp.float32) * SCORE_SCALE
        allowed = (idx_blk[:, None] >= key_index[None, :]) & (seg_blk[:, None] == key_seg[None, :])
        probs = jax.nn.softmax(jnp.where(allowed, scores, -1e30), axis=-1).astype(jnp.bfloat16)
        return jnp.einsum('kgqs,skd->kgqd', probs, v_keys, preferred_element_type=jnp.float32).astype(jnp.bfloat16)

    blocks = (q_rot.reshape(n_blocks, blk_rows, n_kv, group_size, HEAD_DIM),
              row_index.reshape(n_blocks, blk_rows), row_seg.reshape(n_blocks, blk_rows))
    return lax.map(one_block, blocks)


def solution(mesh):
    n_tp = mesh.shape['tp']
    tok_spec = P(('dp', 'sp', 'tp'))
    col_spec = P(None, None, 'tp')
    row_spec = P(None, 'tp', None)
    cache_spec = P(None, ('dp', 'sp'), 'tp', None)

    def device_fn(hidden_in, segment_ids, positions, attn_gain, w_q, w_k, w_v, w_o, mlp_gain, w_gate, w_up, w_down):
        tok_local, model_dim = hidden_in.shape
        n_rows = tok_local * n_tp
        n_kv = w_k.shape[2] // HEAD_DIM
        group_size = w_q.shape[2] // HEAD_DIM // n_kv
        row_seg = lax.all_gather(segment_ids, 'tp', tiled=True)
        row_pos = lax.all_gather(positions, 'tp', tiled=True)
        key_seg = lax.all_gather(row_seg, 'sp', tiled=True)
        row_index = lax.axis_index('sp') * n_rows + jnp.arange(n_rows)
        hidden = hidden_in
        k_list = []
        v_list = []
        for layer_idx in range(w_q.shape[0]):
            normed = lax.all_gather(rms_norm(hidden, attn_gain[layer_idx]), 'tp', axis=0, tiled=True)
            q_lin = jnp.dot(normed, w_q[layer_idx], preferred_element_type=jnp.float32).reshape(n_rows, n_kv * group_size, HEAD_DIM)
            k_lin = jnp.dot(normed, w_k[layer_idx], preferred_element_type=jnp.float32).reshape(n_rows, n_kv, HEAD_DIM)
            v_rows = jnp.dot(normed, w_v[layer_idx], preferred_element_type=jnp.float32).astype(jnp.bfloat16).reshape(n_rows, n_kv, HEAD_DIM)
            q_rot = rotary(q_lin, row_pos).astype(jnp.bfloat16).reshape(n_rows, n_kv, group_size, HEAD_DIM)
            k_rows = rotary(k_lin, row_pos).astype(jnp.bfloat16)
            k_keys = lax.all_gather(k_rows, 'sp', axis=0, tiled=True)
            v_keys = lax.all_gather(v_rows, 'sp', axis=0, tiled=True)
            att_out = attention_rows(q_rot, k_keys, v_keys, row_index, row_seg, key_seg)
            wo_heads = w_o[layer_idx].reshape(n_kv, group_size, HEAD_DIM, model_dim)
            part_sum = jnp.einsum('nkgqd,kgdm->nqm', att_out, wo_heads, preferred_element_type=jnp.float32).astype(jnp.bfloat16).reshape(n_rows, model_dim)
            attn_res = lax.psum_scatter(part_sum, 'tp', scatter_dimension=0, tiled=True)
            hidden_mid = (hidden.astype(jnp.float32) + attn_res.astype(jnp.float32)).astype(jnp.bfloat16)
            hidden = mlp_call(layer_idx, hidden_mid, mlp_gain, w_gate, w_up, w_down)
            k_list.append(k_rows)
            v_list.append(v_rows)
        return hidden, jnp.stack(k_list), jnp.stack(v_list)

    return jax.shard_map(device_fn, mesh=mesh,
                         in_specs=(P(('dp', 'sp', 'tp'), None), tok_spec, tok_spec, P(), col_spec, col_spec, col_spec, row_spec, P(), col_spec, col_spec, row_spec),
                         out_specs=(P(('dp', 'sp', 'tp'), None), cache_spec, cache_spec), check_vma=False)
```

```python
import functools
import math
import jax
import jax.numpy as jnp
from jax import lax
from jax.experimental import pallas as pl
from jax.experimental.pallas import tpu as pltpu
from jax.sharding import PartitionSpec as P

HEAD_DIM = 128
HALF = HEAD_DIM // 2
ROPE_BASE = 1e4
NORM_EPS = 1e-5
SCORE_SCALE = HEAD_DIM ** -0.5
NX = 4
CORES = 2
NY = 4
NZ = 4
SEGMENTS = 4
COUNT_ROWS = 16
NCH = 10
PAIR = 2
AHEAD = 3
LAG_FAR = 3
LAG_USE = 2
RS_LAG_D = 2
RS_LAG_T = 6
RS_LAG_F = 12
WG_SLOTS = 2
WD_SLOTS = 4
VMEM_LIMIT = 63 * 1024 * 1024
BIG = 1e9
NEG = -1e30
MESH = pl.DeviceIdType.MESH
F32 = jnp.float32
BF16 = jnp.bfloat16
LEFT, RIGHT, FAR, P_OWN, P_LEFT, P_RIGHT, P_FAR, KINDS = range(8)
R_PAIR, R_FAR, R_NOW, R_PASS, R_KINDS = range(5)


def scope(name):
    return jax.named_scope(name)


def remote(ref, dst, send, recv, to):
    return pltpu.make_async_remote_copy(src_ref=ref, dst_ref=dst, send_sem=send, recv_sem=recv, device_id=to, device_id_type=MESH)


class Ring:
    def __init__(self):
        self.tp = lax.axis_index('tp')
        self.x = lax.div(self.tp, CORES)
        self.c = lax.rem(self.tp, CORES)
        self.right, self.left = self.dev(1), self.dev(-1)
        self.partner = {'tp': CORES * self.x + 1 - self.c}

    def at(self, dx):
        return lax.rem(self.x + dx + NX, NX)

    def dev(self, dx):
        return {'tp': CORES * self.at(dx) + self.c}


def sign(j):
    return 1 - 2 * lax.rem(j, 2)


def col(ref, j, width):
    return ref.at[:, pl.ds(pl.multiple_of(j * width, width), width)]


class Gather:
    def __init__(self, ring, buf, send, recv, rows, nch):
        self.g, self.buf, self.send, self.recv, self.rows, self.nch = ring, buf, send, recv, rows, nch

    def block(self, j, dx, core):
        r = pl.multiple_of((CORES * self.g.at(dx) + core) * self.rows, self.rows)
        return self.buf.at[j, pl.ds(r, self.rows), :]

    def copy(self, j, kind, dx, to):
        ref = self.block(j, dx, self.g.c)
        return remote(ref, ref, self.send.at[kind, j], self.recv.at[kind, j], to)

    def wait(self, j, kind):
        self.copy(j, kind, 0, self.g.partner).wait_recv()

    def start(self, j):
        self.copy(j, LEFT, 0, self.g.right).start()
        self.copy(j, RIGHT, 0, self.g.left).start()
        self.copy(j, P_OWN, 0, self.g.partner).start()

    def forward(self, j):
        self.wait(j, LEFT)
        self.wait(j, RIGHT)
        way = sign(j)
        self.copy(j, FAR, -way, self.g.dev(way)).start()
        self.copy(j, P_LEFT, -1, self.g.partner).start()
        self.copy(j, P_RIGHT, 1, self.g.partner).start()

    def forward_far(self, j):
        self.wait(j, FAR)
        self.copy(j, P_FAR, 2, self.g.partner).start()

    def drain(self):
        def body(j, _):
            for kind in range(KINDS):
                self.copy(j, kind, 0, self.g.partner).wait_send()
            return 0
        lax.fori_loop(0, self.nch, body, 0)

    def run(self, use, last):
        nch = self.nch
        for j in range(AHEAD):
            self.start(j)

        def whole(t):
            for i in range(PAIR):
                for kind in (P_OWN, P_LEFT, P_RIGHT, P_FAR):
                    self.wait(PAIR * t + i, kind)

        def body(t, _):
            for i in range(PAIR):
                s = PAIR * t + i

                @pl.when(s < nch)
                def _():
                    with scope('ag_fwd'):
                        self.forward(s)

                @pl.when(s + AHEAD < nch)
                def _():
                    self.start(s + AHEAD)

                @pl.when((s >= LAG_FAR) & (s - LAG_FAR < nch))
                def _():
                    with scope('ag_far'):
                        self.forward_far(s - LAG_FAR)

            @pl.when((t >= LAG_USE) & (t - LAG_USE < nch // PAIR - 1))
            def _():
                with scope('ag_whole'):
                    whole(t - LAG_USE)
                with scope('ag_use'):
                    use(t - LAG_USE)
            return 0
        lax.fori_loop(0, max(nch // PAIR - 1 + LAG_USE, pl.cdiv(nch + LAG_FAR, PAIR)), body, 0)
        with scope('ag_whole'):
            whole(nch // PAIR - 1)
        with scope('ag_last'):
            last()
        self.drain()


class Scatter:
    def __init__(self, ring, part, pair, passing, ends, own, out, send, recv, nch):
        self.g, self.part, self.pair, self.passing, self.ends, self.own, self.out = ring, part, pair, passing, ends, own, out
        self.send, self.recv, self.nch = send, recv, nch

    def copy(self, j, kind, src, dst, to):
        return remote(src, dst, self.send.at[kind, j], self.recv.at[kind, j], to)

    def pair_copy(self, j):
        return self.copy(j, R_PAIR, self.part.at[j, :, 1 - self.g.c], self.pair.at[j], self.g.partner)

    def near_copy(self, j, kind, way):
        side = lax.div(1 - way, 2)
        return self.copy(j, kind, self.out.at[j, side], self.ends.at[j, side], self.g.dev(way))

    def far_copy(self, j):
        return self.copy(j, R_FAR, self.out.at[j, 2], self.passing.at[j], self.g.dev(sign(j)))

    def stage_pair(self, j):
        self.pair_copy(j).wait_recv()
        g = self.g

        def both(dx):
            xx = g.at(dx)
            return self.part[j, xx, g.c].astype(F32) + self.pair[j, xx].astype(F32)
        self.out[j, 2] = both(2).astype(BF16)
        self.far_copy(j).start()
        self.out[j, 0] = both(1).astype(BF16)
        self.out[j, 1] = both(-1).astype(BF16)
        self.near_copy(j, R_NOW, -sign(j)).start()
        self.own[j] = both(0)

    def stage_pass(self, j):
        self.far_copy(j).wait_recv()
        side = lax.rem(j, 2)
        self.out[j, side] = (self.out[j, side].astype(F32) + self.passing[j].astype(F32)).astype(BF16)
        self.near_copy(j, R_PASS, sign(j)).start()

    def stage_end(self, j):
        for kind in (R_NOW, R_PASS):
            self.near_copy(j, kind, 1).wait_recv()
        return self.own[j] + self.ends[j, 0].astype(F32) + self.ends[j, 1].astype(F32)

    def drain(self):
        def body(j, _):
            self.pair_copy(j).wait_send()
            for kind in (R_FAR, R_NOW, R_PASS):
                self.near_copy(j, kind, 1).wait_send()
            return 0
        lax.fori_loop(0, self.nch, body, 0)

    def run(self, compute, finish):
        nch = self.nch

        def body(s, _):
            @pl.when(s < nch)
            def _():
                with scope('rs_compute'):
                    self.part[s] = compute(s)
                    self.pair_copy(s).start()

            @pl.when((s >= RS_LAG_D) & (s - RS_LAG_D < nch))
            def _():
                with scope('rs_pair'):
                    self.stage_pair(s - RS_LAG_D)

            @pl.when((s >= RS_LAG_T) & (s - RS_LAG_T < nch))
            def _():
                with scope('rs_pass'):
                    self.stage_pass(s - RS_LAG_T)

            @pl.when(s >= RS_LAG_F)
            def _():
                j = s - RS_LAG_F
                with scope('rs_end'):
                    finish(j, self.stage_end(j))
            return 0
        lax.fori_loop(0, nch + RS_LAG_F, body, 0)
        self.drain()


class Plane:
    def __init__(self):
        self.b = lax.axis_index('sp')
        self.z = lax.div(self.b, NY)
        self.y = lax.rem(self.b, NY)

    def index(self, first_y, df, ds):
        dy, dz = (df, ds) if first_y else (ds, df)
        return lax.rem(self.z + dz + NZ, NZ) * NY + lax.rem(self.y + dy + NY, NY)


class Spread:
    NEAR, STEPS = 3, 6
    FIRST = (0, -1, 1, 2)
    KINDS = NEAR + 3 * len(FIRST)

    def __init__(self, plane, first_y, view, send, recv):
        self.p, self.first_y, self.view, self.send, self.recv = plane, first_y, view, send, recv

    def copy(self, kind, df, ds, to_f, to_s):
        ref = self.view(self.p.index(self.first_y, df, ds))
        return remote(ref, ref, self.send(kind), self.recv(kind), {'sp': self.p.index(self.first_y, to_f, to_s)})

    def put(self, *a):
        self.copy(*a).start()

    def get(self, kind):
        self.copy(kind, 0, 0, 0, 1).wait_recv()

    def across(self, i):
        kind = self.NEAR + 3 * i
        self.put(kind, self.FIRST[i], 0, 0, 1)
        self.put(kind + 1, self.FIRST[i], 0, 0, -1)

    def far(self, i):
        kind = self.NEAR + 3 * i
        self.get(kind)
        self.get(kind + 1)
        way = 1 - 2 * (i % 2)
        self.put(kind + 2, self.FIRST[i], -way, 0, way)

    def step(self, n):
        if n == 0:
            self.put(0, 0, 0, 1, 0)
            self.put(1, 0, 0, -1, 0)
            self.across(0)
        elif n == 1:
            self.get(0)
            self.get(1)
            way = 1 if self.first_y else -1
            self.put(2, -way, 0, way, 0)
            self.across(1)
            self.across(2)
            self.far(0)
        elif n == 2:
            self.get(2)
            self.across(3)
        elif n == 3:
            self.far(1)
            self.far(2)
        elif n == 4:
            self.far(3)
        else:
            for i in range(len(self.FIRST)):
                self.get(self.NEAR + 3 * i + 2)

    def drain(self):
        for kind in range(self.KINDS):
            self.copy(kind, 0, 0, 0, 1).wait_send()


def enter(peers):
    barrier = pltpu.get_barrier_semaphore()
    for dev in peers:
        pl.semaphore_signal(barrier, inc=1, device_id=dev, device_id_type=MESH)
    pl.semaphore_wait(barrier, len(peers))


def joined(parts, axis=0):
    return parts[0] if len(parts) == 1 else jnp.concatenate(parts, axis=axis)


def stack_kernel(dims, x_hbm, aux_hbm, ga_ref, gm_ref, wq_hbm, wk_hbm, wv_hbm, wo_hbm, wg_hbm, wu_hbm, wd_hbm, out_ref, kc_ref, vc_ref,
                 x_ref, gains, aux, nbuf, wq, wkv, wo, qbuf, kbuf, vbuf, segq, sbuf, acc, m_ref, l_ref, obuf,
                 acc_g, acc_u, act, wgu, wd, part, pair, passing, ends, own, outs,
                 in_sem, wq_sem, wo_sem, gu_sem, wd_sem, c_sem, ag_send, ag_recv, ax_send, ax_recv, rs_send, rs_recv, kv_send, kv_recv):
    layers, rows, d_model, heads, units = dims
    cw = d_model // NCH
    chip = CORES * rows
    tokens = NX * chip
    g = Ring()
    p = Plane()
    me = pl.ds(pl.multiple_of(g.tp * rows, rows), rows)

    def attn_weights(layer):
        return [pltpu.make_async_copy(w.at[layer], to, wq_sem.at[i]) for i, (w, to) in enumerate(
            ((wk_hbm, wkv.at[:, pl.ds(0, HEAD_DIM)]), (wv_hbm, wkv.at[:, pl.ds(HEAD_DIM, HEAD_DIM)]), (wq_hbm, wq)))]

    def out_weights(layer):
        return [pltpu.make_async_copy(wo_hbm.at[layer, :, pl.ds(j * cw, cw)], wo.at[j], wo_sem.at[j]) for j in range(NCH)]

    def gu_copies(t):
        slot = lax.rem(t, WG_SLOTS)
        steps = NCH // PAIR
        r = pl.ds(pl.multiple_of(lax.rem(t, steps) * (PAIR * cw), PAIR * cw), PAIR * cw)
        return [pltpu.make_async_copy(w.at[lax.div(t, steps), r, :], wgu.at[slot, k], gu_sem.at[slot, k]) for k, w in enumerate((wg_hbm, wu_hbm))]

    def wd_copy(t):
        slot = lax.rem(t, WD_SLOTS)
        r = pl.ds(pl.multiple_of(lax.rem(t, NCH) * cw, cw), cw)
        return pltpu.make_async_copy(wd_hbm.at[lax.div(t, NCH), :, r], wd.at[slot], wd_sem.at[slot])

    def start_all(copies):
        for w in copies:
            w.start()

    def wait_all(copies):
        for w in copies:
            w.wait()

    first_in = [pltpu.make_async_copy(x_hbm, x_ref, in_sem.at[0]), pltpu.make_async_copy(aux_hbm, aux.at[0, me, :], in_sem.at[1])]
    start_all(first_in)
    start_all(attn_weights(0))
    start_all(out_weights(0))
    for t in range(WG_SLOTS):
        start_all(gu_copies(t))
    for t in range(WD_SLOTS):
        wd_copy(t).start()
    for i, ref in enumerate((ga_ref, gm_ref)):
        for layer in range(layers):
            gains[layer, i] = ref[layer:layer + 1, :].astype(F32)
    with scope('enter'):
        enter([g.right, g.left, g.partner] + [{'sp': p.index(True, df, ds)} for df, ds in ((1, 0), (-1, 0), (0, 1), (0, -1))])
        wait_all(first_in)

    ag = Gather(g, nbuf, ag_send, ag_recv, rows, NCH)
    ax = Gather(g, aux, ax_send, ax_recv, rows, 1)
    rs = Scatter(g, part, pair, passing, ends, own, outs, rs_send, rs_recv, NCH)
    half = lax.div(g.x, 2)
    par = lax.rem(g.x, 2)
    groups = ([(half, par)], [(0, 1 - par), (1, 1 - par)], [(1 - half, par)])
    NEXT = 1

    def norm(layer, which):
        with scope('norm'):
            x32 = x_ref[...].astype(F32)
            inv = lax.rsqrt(jnp.mean(x32 * x32, axis=-1, keepdims=True) + NORM_EPS)
            for j in range(NCH):
                sl = slice(j * cw, (j + 1) * cw)
                nbuf[j, me, :] = (x_ref[:, sl].astype(F32) * inv * gains[layer, which, :, sl]).astype(BF16)

    def finish(j, total):
        x_col = col(x_ref, j, cw)
        x_col[...] = (x_col[...].astype(F32) + total.astype(BF16).astype(F32)).astype(BF16)

    def chip_rows(ip):
        return pl.ds(pl.multiple_of((2 * ip[0] + ip[1]) * chip, chip), chip)

    def project(layer, grp):
        with scope('qkv%d' % grp):
            where = [chip_rows(ip) for ip in groups[grp]]
            q = k_v = None
            for j in range(NCH):
                lhs = joined([nbuf[j, r, :] for r in where])
                dq = jnp.dot(lhs, wq[j * cw:(j + 1) * cw, :], preferred_element_type=F32)
                dkv = jnp.dot(lhs, wkv[j * cw:(j + 1) * cw, :], preferred_element_type=F32)
                q = dq if q is None else q + dq
                k_v = dkv if k_v is None else k_v + dkv
            cosf = joined([aux[0, r, 0:HEAD_DIM] for r in where])
            sinf = joined([aux[0, r, HEAD_DIM:2 * HEAD_DIM] for r in where])

            def rope(v):
                return (v * cosf + pltpu.roll(v, HALF, 1) * sinf).astype(BF16)
            k_new = rope(k_v[:, :HEAD_DIM])
            v_new = k_v[:, HEAD_DIM:].astype(BF16)
            for i, (a, b) in enumerate(groups[grp]):
                sl = slice(i * chip, (i + 1) * chip)
                kbuf[layer, p.b, a, b, 0:chip] = k_new[sl]
                vbuf[layer, p.b, a, b] = v_new[sl]
                seg = aux[0, where[i], 2 * HEAD_DIM:3 * HEAD_DIM]
                counts = [jnp.sum(jnp.where(seg < float(v), 1.0, 0.0), axis=0, keepdims=True) for v in range(SEGMENTS)]
                kbuf[layer, p.b, a, b, chip:] = joined(counts + [jnp.zeros((COUNT_ROWS - SEGMENTS, HEAD_DIM), F32)]).astype(BF16)
            for h in range(heads):
                q_new = rope(q[:, h * HEAD_DIM:(h + 1) * HEAD_DIM])
                for i, r in enumerate(where):
                    qbuf[h, r, :] = q_new[i * chip:(i + 1) * chip]

    scale = SCORE_SCALE * math.log2(math.e)

    def scores(layer, zz, ip, slot):
        first = (2 * ip[0] + ip[1]) * chip
        keytok = lax.broadcasted_iota(jnp.int32, (chip, tokens), 0).astype(F32)
        qtok = (lax.broadcasted_iota(jnp.int32, (1, tokens), 1) - first).astype(F32)
        seg = segq[0:1, :]
        keys = kbuf[layer, pl.ds(zz * NY, NY), ip[0], ip[1], 0:chip].reshape(NY * chip, HEAD_DIM)
        raw = [lax.dot_general(keys, qbuf[h], (((1,), (1,)), ((), ())), preferred_element_type=F32) for h in range(heads)]
        for yy in range(NY):
            blk = zz * NY + yy
            cb = kbuf[layer, blk, ip[0], ip[1], chip:].astype(F32)
            low = jnp.zeros((1, tokens), F32)
            for v in range(1, SEGMENTS):
                n_v = joined([cb[v:v + 1]] * (tokens // HEAD_DIM), axis=1)
                low = low + jnp.where(seg == float(v), n_v, 0.0)
            rel = blk - p.b
            past = jnp.where(rel < 0, BIG, jnp.where(rel > 0, -BIG, 0.0))
            here = jnp.where(rel == 0, 1.0, 0.0)
            high = past + here * qtok
            bias = jnp.where((keytok >= low) & (keytok <= high), 0.0, NEG)
            sl = slice(yy * chip, (yy + 1) * chip)
            for h in range(heads):
                sbuf[slot, h, sl, :] = raw[h][sl] * scale + bias

    def absorb(layer, zz, ip, slot):
        vals_t = vbuf[layer, pl.ds(zz * NY, NY), ip[0], ip[1]].reshape(NY * chip, HEAD_DIM).T
        for h in range(heads):
            s = sbuf[slot, h]
            m_old = m_ref[h]
            m_new = jnp.maximum(m_old, jnp.max(s, axis=0, keepdims=True))
            alpha = jnp.exp2(m_old - m_new)
            w = jnp.exp2(s - m_new)
            l_ref[h] = l_ref[h] * alpha + jnp.sum(w, axis=0, keepdims=True)
            m_ref[h] = m_new
            acc[h] = acc[h] * alpha + jnp.dot(vals_t, w.astype(BF16), preferred_element_type=F32)

    def attend(layer, grp):
        chips = groups[grp]
        n = len(chips)
        total = (p.z + 1) * n

        def place(t):
            if n == 1:
                return t, chips[0]
            return lax.div(t, n), (lax.rem(t, n), chips[0][1])

        with scope('attend%d' % grp):
            scores(layer, *place(0), 0)

            def body(t, _):
                slot = lax.rem(t, 2)
                scores(layer, *place(lax.min(t + 1, total - 1)), 1 - slot)
                absorb(layer, *place(t), slot)
                return 0
            lax.fori_loop(0, total, body, 0)

    def attention_phase(layer):
        def view(buf, grp):
            if grp == NEXT:
                return lambda b: buf.at[layer, b, :, 1 - par]
            return lambda b: buf.at[layer, b, groups[grp][0][0], par]
        kv = [[Spread(p, buf is kbuf, view(buf, grp), (lambda kind, at=(grp, k): kv_send.at[layer, at[0], at[1], kind]),
                      (lambda kind, at=(grp, k): kv_recv.at[layer, at[0], at[1], kind]))
               for k, buf in enumerate((kbuf, vbuf))] for grp in range(len(groups))]

        def kv_step(grp, n):
            with scope('kv%d_%d' % (grp, n)):
                for s in kv[grp]:
                    s.step(n)

        def wait(*kinds):
            with scope('wait%d' % kinds[0]):
                for j in range(NCH):
                    for kind in kinds:
                        ag.wait(j, kind)

        def aux_wait(*kinds):
            @pl.when(layer == 0)
            def _():
                for kind in kinds:
                    ax.wait(0, kind)

        def fwd(lo, hi):
            with scope('fwd'):
                for j in range(lo, hi):
                    ag.forward(j)

        @pl.when(layer == 0)
        def _():
            ax.start(0)
        norm(layer, 0)
        early = AHEAD + 1
        for j in range(early):
            ag.start(j)
        aux_wait(P_OWN)
        for j in range(early, NCH):
            ag.copy(j, P_OWN, 0, g.partner).start()
        wait(P_OWN)
        wait_all(attn_weights(layer))
        project(layer, 0)
        kv_step(0, 0)

        @pl.when(layer == 0)
        def _():
            ax.forward(0)
        for j in range(early, NCH):
            ag.copy(j, LEFT, 0, g.right).start()
            ag.copy(j, RIGHT, 0, g.left).start()
        fwd(0, early)
        kv_step(0, 1)
        fwd(early, NCH - AHEAD)

        @pl.when(layer == 0)
        def _():
            ax.forward_far(0)
        kv_step(0, 2)
        kv_step(0, 3)
        fwd(NCH - AHEAD, NCH)
        wait(P_LEFT, P_RIGHT)
        aux_wait(P_LEFT, P_RIGHT)
        project(layer, NEXT)
        kv_step(NEXT, 0)
        kv_step(0, 4)
        with scope('fwd_far'):
            for j in range(NCH):
                ag.forward_far(j)
        kv_step(NEXT, 1)
        wait(P_FAR)

        @pl.when(layer == 0)
        def _():
            ax.wait(0, P_FAR)
            segq[...] = aux[0, :, 2 * HEAD_DIM:3 * HEAD_DIM].T[0:segq.shape[0], :]
        project(layer, 2)
        kv_step(2, 0)

        @pl.when(layer + 1 < layers)
        def _():
            start_all(attn_weights(layer + 1))
        kv_step(NEXT, 2)
        kv_step(0, 5)
        acc[...] = jnp.zeros_like(acc)
        l_ref[...] = jnp.zeros_like(l_ref)
        m_ref[...] = jnp.full_like(m_ref, NEG)
        attend(layer, 0)
        kv_step(NEXT, 3)
        kv_step(2, 1)
        kv_step(NEXT, 4)
        kv_step(2, 2)
        kv_step(2, 3)
        kv_step(NEXT, 5)
        attend(layer, NEXT)
        kv_step(2, 4)
        kv_step(2, 5)
        attend(layer, 2)
        with scope('heads'):
            for h in range(heads):
                obuf[:, h * HEAD_DIM:(h + 1) * HEAD_DIM] = (acc[h] / l_ref[h]).T.astype(BF16)
            caches = [pltpu.make_async_copy(kbuf.at[layer, p.b, :, :, pl.ds(0, chip)], kc_ref.at[layer], c_sem.at[0]),
                      pltpu.make_async_copy(vbuf.at[layer, p.b], vc_ref.at[layer], c_sem.at[1])]
            start_all(caches)
            ag.drain()
            wait_all(out_weights(layer))

        def proj_out(j):
            return jnp.dot(obuf[...], wo[j], preferred_element_type=F32).astype(BF16).reshape(NX, CORES, rows, cw)
        rs.run(proj_out, finish)
        with scope('drain'):
            @pl.when(layer + 1 < layers)
            def _():
                start_all(out_weights(layer + 1))

            @pl.when(layer == 0)
            def _():
                ax.drain()
            for grp in kv:
                for s in grp:
                    s.drain()
            wait_all(caches)

    def mlp_phase(layer):
        steps = NCH // PAIR
        norm(layer, 1)
        acc_g[...] = jnp.zeros_like(acc_g)
        acc_u[...] = jnp.zeros_like(acc_u)

        def lhs(t, i):
            return nbuf[PAIR * t + i]

        def refill(t):
            @pl.when(t + WG_SLOTS < layers * steps)
            def _():
                start_all(gu_copies(t + WG_SLOTS))

        def half_dot(t, k, slot, sl):
            return sum(jnp.dot(lhs(t, i), wgu[slot, k, i * cw:(i + 1) * cw, sl], preferred_element_type=F32) for i in range(PAIR))

        def gate_up(t):
            at = layer * steps + t
            wait_all(gu_copies(at))
            slot = lax.rem(at, WG_SLOTS)
            for k, into in enumerate((acc_g, acc_u)):
                into[...] += half_dot(t, k, slot, slice(None))
            refill(at)

        def gate_up_last():
            t = steps - 1
            at = layer * steps + t
            wait_all(gu_copies(at))
            slot = lax.rem(at, WG_SLOTS)
            step = min(CORES * HEAD_DIM, units)
            for lo in range(0, units, step):
                sl = slice(lo, lo + step)
                gate = acc_g[:, sl] + half_dot(t, 0, slot, sl)
                up = acc_u[:, sl] + half_dot(t, 1, slot, sl)
                act[:, sl] = (gate * jax.nn.sigmoid(gate) * up).astype(BF16)
            refill(at)

        ag.run(gate_up, gate_up_last)

        def down(j):
            at = layer * NCH + j
            wd_copy(at).wait()
            res = jnp.dot(act[...], wd[lax.rem(at, WD_SLOTS)], preferred_element_type=F32).astype(BF16)

            @pl.when(at + WD_SLOTS < layers * NCH)
            def _():
                wd_copy(at + WD_SLOTS).start()
            return res.reshape(NX, CORES, rows, cw)
        rs.run(down, finish)

    def layer_body(layer, _):
        attention_phase(layer)
        mlp_phase(layer)
        return 0
    lax.fori_loop(0, layers, layer_body, 0)
    out_ref[...] = x_ref[...]


def stack_call(hidden, aux, attn_gain, mlp_gain, w_q, w_k, w_v, w_o, w_gate, w_up, w_down):
    rows, d_model = hidden.shape
    layers = w_q.shape[0]
    cw = d_model // NCH
    q_dim, units = w_q.shape[2], w_gate.shape[2]
    heads = q_dim // HEAD_DIM
    chip = CORES * rows
    tokens = NX * chip
    blocks = NY * NZ
    hbm = pl.BlockSpec(memory_space=pl.ANY)
    vmem = pl.BlockSpec(memory_space=pltpu.VMEM)
    dma = pltpu.SemaphoreType.DMA
    cache = jax.ShapeDtypeStruct((layers, 2, 2, chip, HEAD_DIM), BF16)

    def b16(*shape):
        return pltpu.VMEM(shape, BF16)

    def f32(*shape):
        return pltpu.VMEM(shape, F32)
    out, k_c, v_c = pl.pallas_call(
        functools.partial(stack_kernel, (layers, rows, d_model, heads, units)),
        out_shape=(jax.ShapeDtypeStruct((rows, d_model), BF16), cache, cache),
        in_specs=[hbm, hbm, vmem, vmem] + [hbm] * 7,
        out_specs=(vmem, hbm, hbm),
        scratch_shapes=[
            b16(rows, d_model), f32(layers, 2, 1, d_model), f32(1, tokens, 3 * HEAD_DIM), b16(NCH, tokens, cw),
            b16(d_model, q_dim), b16(d_model, 2 * HEAD_DIM), b16(NCH, q_dim, cw), b16(heads, tokens, HEAD_DIM),
            b16(layers, blocks, 2, 2, chip + COUNT_ROWS, HEAD_DIM), b16(layers, blocks, 2, 2, chip, HEAD_DIM),
            f32(8, tokens), f32(2, heads, NY * chip, tokens), f32(heads, HEAD_DIM, tokens), f32(heads, 1, tokens), f32(heads, 1, tokens),
            b16(tokens, q_dim),
            f32(tokens, units), f32(tokens, units), b16(tokens, units), b16(WG_SLOTS, 2, PAIR * cw, units), b16(WD_SLOTS, units, cw),
            b16(NCH, NX, CORES, rows, cw), b16(NCH, NX, rows, cw), b16(NCH, rows, cw), b16(NCH, 2, rows, cw), f32(NCH, rows, cw),
            b16(NCH, 3, rows, cw),
            dma((2,)), dma((3,)), dma((NCH,)), dma((WG_SLOTS, 2)), dma((WD_SLOTS,)), dma((2,)),
            dma((KINDS, NCH)), dma((KINDS, NCH)), dma((KINDS, 1)), dma((KINDS, 1)), dma((R_KINDS, NCH)), dma((R_KINDS, NCH)),
            dma((layers, 3, 2, Spread.KINDS)), dma((layers, 3, 2, Spread.KINDS)),
        ],
        compiler_params=pltpu.CompilerParams(collective_id=0, has_side_effects=True, vmem_limit_bytes=VMEM_LIMIT),
        name='stack',
    )(hidden, aux, attn_gain, mlp_gain, w_q, w_k, w_v, w_o, w_gate, w_up, w_down)
    return out, k_c.reshape(layers, tokens, 1, HEAD_DIM), v_c.reshape(layers, tokens, 1, HEAD_DIM)


def aux_table(positions, segment_ids):
    inv_freq = ROPE_BASE ** (-jnp.arange(HALF, dtype=jnp.float32) / HALF)
    angles = positions.astype(jnp.float32)[:, None] * inv_freq
    cos_val = jnp.cos(angles)
    sin_val = jnp.sin(angles)
    seg = jnp.broadcast_to(segment_ids.astype(F32)[:, None], (positions.shape[0], HEAD_DIM))
    return jnp.concatenate([cos_val, cos_val, -sin_val, sin_val, seg], axis=-1)


def solution(mesh):
    tok_spec = P(('dp', 'sp', 'tp'))
    row_block = P(('dp', 'sp', 'tp'), None)
    col_spec = P(None, None, 'tp')
    row_spec = P(None, 'tp', None)
    cache_spec = P(None, ('dp', 'sp'), 'tp', None)

    def device_fn(hidden_in, segment_ids, positions, attn_gain, w_q, w_k, w_v, w_o, mlp_gain, w_gate, w_up, w_down):
        aux = aux_table(positions, segment_ids)
        return stack_call(hidden_in, aux, attn_gain, mlp_gain, w_q, w_k, w_v, w_o, w_gate, w_up, w_down)

    return jax.shard_map(device_fn, mesh=mesh,
                         in_specs=(row_block, tok_spec, tok_spec, P(), col_spec, col_spec, col_spec, row_spec, P(), col_spec, col_spec, row_spec),
                         out_specs=(row_block, cache_spec, cache_spec), check_vma=False)
```
